32 devices in a mesh: dp: 16 (over z, y, x), tensor: 2 (over core).
Axes of the slice: x: 2, y: 2, z: 4, core: 2. Of those that a mesh axis runs over, the one named last changes fastest.
Arguments:
- x_in: float32 [32768, 1024], P(('dp', 'tensor')), may hold values from -6 to 6
- segment_ids: int32 [32768], P('dp'), may hold values from 0 to 31, never falling along the last dimension, each value on 1 to 2000 neighbouring positions
- cotangent: float32 [32768, 1024], P(('dp', 'tensor')), may hold values from -6 to 6
- gain_mix: float32 [1024], replicated, may hold values from 0.5 to 1.5
- mean_gain_mix: float32 [1024], replicated, may hold values from -56 to 56
- var_gain_mix: float32 [1024], replicated, may hold values from 1638.4 to 16384
- gain_ffn: float32 [1024], replicated, may hold values from 0.5 to 1.5
- mean_gain_ffn: float32 [1024], replicated, may hold values from -56 to 56
- var_gain_ffn: float32 [1024], replicated, may hold values from 163.84 to 1638.4
- conv_taps: float32 [3, 1024], P(None, 'tensor'), may hold values from -3 to 3
- mean_conv_taps: float32 [3, 1024], P(None, 'tensor'), may hold values from -56 to 56
- var_conv_taps: float32 [3, 1024], P(None, 'tensor'), may hold values from 327.68 to 3276.8
- w_inproj: float32 [3, 1024, 1024], P(None, 'dp', 'tensor'), may hold values from -0.1875 to 0.1875
- mean_w_inproj: float32 [3, 1024, 1024], P(None, 'dp', 'tensor'), may hold values from -56 to 56
- var_w_inproj: float32 [3, 1024, 1024], P(None, 'dp', 'tensor'), may hold values from 327.68 to 3276.8
- w_outproj: float32 [1024, 1024], P('dp', 'tensor'), may hold values from -0.1875 to 0.1875
- mean_w_outproj: float32 [1024, 1024], P('dp', 'tensor'), may hold values from -56 to 56
- var_w_outproj: float32 [1024, 1024], P('dp', 'tensor'), may hold values from 327.68 to 3276.8
- w_gateup: float32 [2, 1024, 4608], P(None, 'dp', 'tensor'), may hold values from -0.1875 to 0.1875
- mean_w_gateup: float32 [2, 1024, 4608], P(None, 'dp', 'tensor'), may hold values from -56 to 56
- var_w_gateup: float32 [2, 1024, 4608], P(None, 'dp', 'tensor'), may hold values from 163.84 to 1638.4
- w_down: float32 [1024, 4608], P('dp', 'tensor'), may hold values from -0.09375 to 0.09375
- mean_w_down: float32 [1024, 4608], P('dp', 'tensor'), may hold values from -56 to 56
- var_w_down: float32 [1024, 4608], P('dp', 'tensor'), may hold values from 163.84 to 1638.4
Outputs:
- block_out: float32 [32768, 1024], P(('dp', 'tensor'))
- grad_x: float32 [32768, 1024], P(('dp', 'tensor'))
- grad_gain_mix: float32 [1024], replicated
- grad_gain_ffn: float32 [1024], replicated
- grad_conv_taps: float32 [3, 1024], P(None, 'tensor')
- grad_w_inproj: float32 [3, 1024, 1024], P(None, 'dp', 'tensor')
- grad_w_outproj: float32 [1024, 1024], P('dp', 'tensor')
- grad_w_gateup: float32 [2, 1024, 4608], P(None, 'dp', 'tensor')
- grad_w_down: float32 [1024, 4608], P('dp', 'tensor')
- new_gain_mix: float32 [1024], replicated
- new_gain_ffn: float32 [1024], replicated
- new_conv_taps: float32 [3, 1024], P(None, 'tensor')
- new_w_inproj: float32 [3, 1024, 1024], P(None, 'dp', 'tensor')
- new_w_outproj: float32 [1024, 1024], P('dp', 'tensor')
- new_w_gateup: float32 [2, 1024, 4608], P(None, 'dp', 'tensor')
- new_w_down: float32 [1024, 4608], P('dp', 'tensor')
- new_mean_gain_mix: float32 [1024], replicated
- new_mean_gain_ffn: float32 [1024], replicated
- new_mean_conv_taps: float32 [3, 1024], P(None, 'tensor')
- new_mean_w_inproj: float32 [3, 1024, 1024], P(None, 'dp', 'tensor')
- new_mean_w_outproj: float32 [1024, 1024], P('dp', 'tensor')
- new_mean_w_gateup: float32 [2, 1024, 4608], P(None, 'dp', 'tensor')
- new_mean_w_down: float32 [1024, 4608], P('dp', 'tensor')
- new_var_gain_mix: float32 [1024], replicated
- new_var_gain_ffn: float32 [1024], replicated
- new_var_conv_taps: float32 [3, 1024], P(None, 'tensor')
- new_var_w_inproj: float32 [3, 1024, 1024], P(None, 'dp', 'tensor')
- new_var_w_outproj: float32 [1024, 1024], P('dp', 'tensor')
- new_var_w_gateup: float32 [2, 1024, 4608], P(None, 'dp', 'tensor')
- new_var_w_down: float32 [1024, 4608], P('dp', 'tensor')
The draws below stay inside these ranges and needn't reach their ends.
Inputs may be any that keep to these rules, and one draw needn't show every extreme that they name: segment_ids never fall along the tokens; every document number from 0 to 31 occurs; a document has 1 to 2000 tokens and one has exactly 2000.
All inputs are finite; a program needn't handle non-finite values.
Results may differ from the reference program's by a relative error of at most 0.033.
Values may be sent and summed in bfloat16 or wider, within the bound.
A program may use at most 320 MiB of HBM per device.

```python
import math
import jax
import jax.numpy as jnp
import numpy as np
from jax import lax

D = 1024
FF = 4608
KW = 3
TOK_DP = 2048
DOC_MOST = 2000
TOKENS = 32768
DOCS = 32
N_DP = 16
N_TENSOR = 2


def with_spikes(array, rng, source, target, shards_of, factor):
    def block_of(position):
        return (jnp.arange(array.shape[position]) // (array.shape[position] // shards_of)).reshape((-1,) + (1,) * (array.ndim - 1 - position))

    near = jax.random.permutation(rng, shards_of)[block_of(target)]
    far = (block_of(target) + shards_of // 2) % shards_of
    return jnp.where((block_of(source) == near) | (block_of(source) == far), factor * array, array)


def block_levels(stream_key, extent, shards, least, high):
    level = 1.0
    for position, blocks in shards:
        steps = jax.random.uniform(jax.random.fold_in(jax.random.fold_in(stream_key, 6), position), (blocks,), jnp.float32, least / len(shards), high / len(shards))
        level = level * jnp.repeat(jnp.exp(steps), extent[position] // blocks).reshape((-1,) + (1,) * (len(extent) - 1 - position))
    return level


def profile(count, total, reach, slope):
    portions = [(1 << 20) // math.isqrt(grade ** slope) + 1 for grade in range(2, count + 1)]
    rest, given = total - reach - (count - 1), [1] * (count - 1)
    while rest > 0:
        movable = [i for i in range(count - 1) if given[i] < reach]
        whole, left = sum([portions[i] for i in movable]), rest
        for i in movable:
            more = min(reach - given[i], max(1, left * portions[i] // whole), rest)
            given[i] = given[i] + more
            rest = rest - more
    return np.array([reach] + given)


def uneven_parts(rng, count, total, most, skew):
    if count == 2:
        one = jax.random.randint(rng, (), max(1, total - most), min(most, total - 1) + 1)
        return jnp.stack([one, total - one])
    lengths = jnp.asarray(profile(count, total, most, skew), jnp.int32)
    couples = (count - 1) // 2
    donor, receiver = lengths[1:1 + 2 * couples:2], lengths[2:2 + 2 * couples:2]
    room = jnp.minimum(donor - 1, most - receiver)
    moved = jax.random.randint(jax.random.fold_in(rng, 1), (couples,), 0, 1 << 20) % (room + 1)
    lengths = lengths.at[1:1 + 2 * couples:2].set(donor - moved).at[2:2 + 2 * couples:2].set(receiver + moved)
    return lengths[jax.random.permutation(jax.random.fold_in(rng, 2), count)]


def normal_values(rng, shape, deviation, bound, shards=(), kind=jnp.bfloat16):
    entries = jax.random.normal(rng, shape, jnp.float32) * deviation
    if len(shards) > 0:
        entries = block_levels(rng, shape, shards, -0.22, 0.18) * entries
    return jnp.clip(entries, min=-bound, max=bound).astype(kind)


def gaussian_with(rng, shape, deviation, most, cuts, heavy, kind=jnp.bfloat16):
    entries = deviation * jax.random.normal(rng, shape, jnp.float32)
    if cuts:
        entries = entries * block_levels(rng, shape, cuts, -0.22, 0.18)
    return jnp.clip(with_spikes(entries, jax.random.fold_in(rng, 3), *heavy), -most, most).astype(kind)


def setup_inputs(seed: int = 0) -> dict:
    key_of = jax.random.split(jax.random.key(seed), 25)
    x_in = gaussian_with(key_of[0], (TOKENS, D), 1.0, 6.0, ((0, 32),), (0, 1, 32, 2.75), jnp.float32)
    segment_ids = jnp.searchsorted(jnp.cumsum(uneven_parts(key_of[1], DOCS, TOKENS, DOC_MOST, 1)), jnp.arange(TOKENS), side="right").astype(jnp.int32)
    cotangent = gaussian_with(key_of[2], (TOKENS, D), 1.0, 6.0, ((0, 32),), (0, 1, 32, 2.75), jnp.float32)
    gain_mix = jnp.clip(1.0 + 0.1 * jax.random.normal(key_of[3], (D,), jnp.float32), 0.5, 1.5)
    mean_gain_mix = normal_values(key_of[4], (D,), (0.05 * TOKENS ** 0.5), 56.0, (), jnp.float32)
    var_gain_mix = jnp.clip(jnp.exp(jax.random.uniform(key_of[5], (D,), jnp.float32, math.log(1638.4), math.log(16384.0))), 1638.4, 16384.0)
    gain_ffn = jnp.clip(1.0 + 0.1 * jax.random.normal(key_of[6], (D,), jnp.float32), 0.5, 1.5)
    mean_gain_ffn = normal_values(key_of[7], (D,), (0.05 * TOKENS ** 0.5), 56.0, (), jnp.float32)
    var_gain_ffn = jnp.clip(jnp.exp(jax.random.uniform(key_of[8], (D,), jnp.float32, math.log(163.84), math.log(1638.4))), 163.84, 1638.4)
    conv_taps = normal_values(key_of[9], (KW, D), 0.6, 3.0, ((1, 2),), jnp.float32)
    mean_conv_taps = normal_values(key_of[10], (KW, D), (0.05 * TOKENS ** 0.5), 56.0, ((1, 2),), jnp.float32)
    var_conv_taps = jnp.clip(jnp.exp(math.log(3276.8) - 2.3025851 * jax.random.uniform(key_of[11], (KW, D), jnp.float32) ** block_levels(key_of[11], (KW, D), ((1, 2),), -0.2, 0.2)), 327.68, 3276.8)
    w_inproj = normal_values(key_of[12], (KW, D, D), D ** -0.5, 0.1875, ((1, 16), (2, 2)), jnp.float32)
    mean_w_inproj = normal_values(key_of[13], (KW, D, D), (0.05 * TOKENS ** 0.5), 56.0, ((1, 16), (2, 2)), jnp.float32)
    var_w_inproj = jnp.clip(jnp.exp(math.log(3276.8) - 2.3025851 * jax.random.uniform(key_of[14], (KW, D, D), jnp.float32) ** block_levels(key_of[14], (KW, D, D), ((1, 16), (2, 2)), -0.2, 0.2)), 327.68, 3276.8)
    w_outproj = normal_values(key_of[15], (D, D), D ** -0.5, 0.1875, ((0, 16), (1, 2)), jnp.float32)
    mean_w_outproj = normal_values(key_of[16], (D, D), (0.05 * TOKENS ** 0.5), 56.0, ((0, 16), (1, 2)), jnp.float32)
    var_w_outproj = jnp.clip(jnp.exp(math.log(3276.8) - 2.3025851 * jax.random.uniform(key_of[17], (D, D), jnp.float32) ** block_levels(key_of[17], (D, D), ((0, 16), (1, 2)), -0.2, 0.2)), 327.68, 3276.8)
    w_gateup = normal_values(key_of[18], (2, D, FF), D ** -0.5, 0.1875, ((1, 16), (2, 2)), jnp.float32)
    mean_w_gateup = normal_values(key_of[19], (2, D, FF), (0.05 * TOKENS ** 0.5), 56.0, ((1, 16), (2, 2)), jnp.float32)
    var_w_gateup = jnp.clip(jnp.exp(math.log(1638.4) - 2.3025851 * jax.random.uniform(key_of[20], (2, D, FF), jnp.float32) ** block_levels(key_of[20], (2, D, FF), ((1, 16), (2, 2)), -0.2, 0.2)), 163.84, 1638.4)
    w_down = normal_values(key_of[21], (D, FF), FF ** -0.5, 0.09375, ((0, 16), (1, 2)), jnp.float32)
    mean_w_down = normal_values(key_of[22], (D, FF), (0.05 * TOKENS ** 0.5), 56.0, ((0, 16), (1, 2)), jnp.float32)
    var_w_down = jnp.clip(jnp.exp(math.log(1638.4) - 2.3025851 * jax.random.uniform(key_of[23], (D, FF), jnp.float32) ** block_levels(key_of[23], (D, FF), ((0, 16), (1, 2)), -0.2, 0.2)), 163.84, 1638.4)
    return dict(x_in=x_in, segment_ids=segment_ids, cotangent=cotangent, gain_mix=gain_mix, mean_gain_mix=mean_gain_mix, var_gain_mix=var_gain_mix, gain_ffn=gain_ffn, mean_gain_ffn=mean_gain_ffn, var_gain_ffn=var_gain_ffn, conv_taps=conv_taps, mean_conv_taps=mean_conv_taps, var_conv_taps=var_conv_taps, w_inproj=w_inproj, mean_w_inproj=mean_w_inproj, var_w_inproj=var_w_inproj, w_outproj=w_outproj, mean_w_outproj=mean_w_outproj, var_w_outproj=var_w_outproj, w_gateup=w_gateup, mean_w_gateup=mean_w_gateup, var_w_gateup=var_w_gateup, w_down=w_down, mean_w_down=mean_w_down, var_w_down=var_w_down)


norm_eps = 1e-05
beta_one = 0.9
beta_two = 0.95
adam_eps = 1e-08
rate_matrix = 0.02
rate_small = 0.2
decay_matrix = 0.1
bias_one = 1.0 - 0.9 ** 3
bias_two = 1.0 - 0.95 ** 3

def to_bf16(values):
    return lax.optimization_barrier(values.astype(jnp.bfloat16))

def rms_scale(values):
    return lax.rsqrt(lax.optimization_barrier(jnp.mean(values * values, axis=1, keepdims=True)) + norm_eps)

def norm_back(d_normed, values, scale_rows, gain):
    gain_part = lax.optimization_barrier(jnp.sum(d_normed * values * scale_rows, axis=0))
    scaled = d_normed * gain
    inner = lax.optimization_barrier(jnp.mean(scaled * values, axis=1, keepdims=True))
    return (scale_rows * (scaled - values * scale_rows * scale_rows * inner), gain_part)

def adamw(weight, gradient, moment, square, step_size, weight_decay):
    new_moment = beta_one * moment + (1.0 - beta_one) * gradient
    new_square = beta_two * square + (1.0 - beta_two) * gradient * gradient
    direction = new_moment / bias_one / (jnp.sqrt(new_square / bias_two) + adam_eps)
    return (weight - step_size * (direction + weight_decay * weight), new_moment, new_square)

def tensor_sum(pairs, width):
    running_sum = None
    for group_index in range(N_TENSOR):
        first_col = group_index * width
        block_term = None
        for left_rows, right_rows in pairs:
            product = jnp.dot(left_rows[:, first_col:first_col + width], right_rows[:, first_col:first_col + width].T, preferred_element_type=jnp.float32)
            block_term = product if block_term is None else block_term + product
        rounded = to_bf16(block_term).astype(jnp.float32)
        running_sum = rounded if running_sum is None else running_sum + rounded
    return running_sum

def conv_terms(mixed_rows, prev_u, ids_float, prev_ids):
    token_count = mixed_rows.shape[0]
    ext_u = jnp.concatenate([prev_u, mixed_rows], axis=0)
    ext_ids = jnp.concatenate([prev_ids, ids_float], axis=0)
    same_one = (ext_ids[1:token_count + 1] == ids_float).astype(jnp.float32)[:, None]
    same_two = (ext_ids[0:token_count] == ids_float).astype(jnp.float32)[:, None]
    return (ext_u[1:token_count + 1], ext_u[0:token_count], same_one, same_two)

def conv_back(d_conv, conv_taps, same_one, same_two):
    token_count = d_conv.shape[0]
    term_zero = conv_taps[0] * d_conv
    term_one = conv_taps[1] * same_one * d_conv
    term_two = conv_taps[2] * same_two * d_conv
    zero_rows = jnp.zeros((2, d_conv.shape[1]), d_conv.dtype)
    local_grad = term_zero + jnp.concatenate([term_one, zero_rows], axis=0)[1:token_count + 1] + jnp.concatenate([term_two, zero_rows], axis=0)[2:token_count + 2]
    edge_out = jnp.stack([term_two[0], term_one[0] + term_two[1]])
    return (local_grad, edge_out)

def add_edge(local_grad, edge_in):
    token_count = local_grad.shape[0]
    filler = jnp.zeros((token_count - 2, local_grad.shape[1]), local_grad.dtype)
    return local_grad + jnp.concatenate([filler, edge_in], axis=0)

def reference(x_in, segment_ids, cotangent, gain_mix, mean_gain_mix, var_gain_mix, gain_ffn, mean_gain_ffn, var_gain_ffn, conv_taps, mean_conv_taps, var_conv_taps, w_inproj, mean_w_inproj, var_w_inproj, w_outproj, mean_w_outproj, var_w_outproj, w_gateup, mean_w_gateup, var_w_gateup, w_down, mean_w_down, var_w_down):
    w_in_b = w_inproj.astype(jnp.bfloat16)
    w_out_b = w_outproj.astype(jnp.bfloat16)
    w_gu_b = w_gateup.astype(jnp.bfloat16)
    w_down_b = w_down.astype(jnp.bfloat16)
    chan_width = D // N_TENSOR
    hidden_width = FF // N_TENSOR
    x_blocks = x_in.reshape(N_DP, TOK_DP, D)
    cot_blocks = cotangent.reshape(N_DP, TOK_DP, D)
    id_blocks = segment_ids.reshape(N_DP, TOK_DP).astype(jnp.float32)
    before_rows_all = jnp.concatenate([jnp.zeros((1, 2, D), x_in.dtype), x_blocks[:-1, TOK_DP - 2:]], axis=0)
    before_ids_all = jnp.concatenate([jnp.zeros((1, 2), id_blocks.dtype), id_blocks[:-1, TOK_DP - 2:]], axis=0)

    def block_step(carry, inputs):
        edge_in, sums_in = carry
        x_rows, id_rows, cot_rows, before_rows, before_ids = inputs
        scale_before = rms_scale(before_rows)
        normed_before = to_bf16(before_rows * scale_before * gain_mix)
        prev_u = jnp.dot(normed_before, w_in_b[0], preferred_element_type=jnp.float32) * jnp.dot(normed_before, w_in_b[2], preferred_element_type=jnp.float32)
        scale_mix = rms_scale(x_rows)
        normed_mix = to_bf16(x_rows * scale_mix * gain_mix)
        gate_b = jnp.dot(normed_mix, w_in_b[0], preferred_element_type=jnp.float32)
        gate_c = jnp.dot(normed_mix, w_in_b[1], preferred_element_type=jnp.float32)
        gate_x = jnp.dot(normed_mix, w_in_b[2], preferred_element_type=jnp.float32)
        mixed_rows = gate_b * gate_x
        shift_one, shift_two, same_one, same_two = conv_terms(mixed_rows, prev_u, id_rows, before_ids)
        conv_out = conv_taps[0] * mixed_rows + conv_taps[1] * same_one * shift_one + conv_taps[2] * same_two * shift_two
        gated = to_bf16(gate_c * conv_out)
        residual = x_rows + tensor_sum([(gated, w_out_b)], chan_width)
        scale_ffn = rms_scale(residual)
        normed_ffn = to_bf16(residual * scale_ffn * gain_ffn)
        gate_pre = jnp.dot(normed_ffn, w_gu_b[0], preferred_element_type=jnp.float32)
        up_pre = jnp.dot(normed_ffn, w_gu_b[1], preferred_element_type=jnp.float32)
        sigmoid_gate = jax.nn.sigmoid(gate_pre)
        activated = to_bf16(gate_pre * sigmoid_gate * up_pre)
        block_rows = residual + tensor_sum([(activated, w_down_b)], hidden_width)
        cot_b = to_bf16(cot_rows)
        d_act = jnp.dot(cot_b, w_down_b, preferred_element_type=jnp.float32)
        g_down = jnp.dot(cot_b.T, activated, preferred_element_type=jnp.float32)
        d_gate = to_bf16(d_act * up_pre * sigmoid_gate * (1.0 + gate_pre * (1.0 - sigmoid_gate)))
        d_up = to_bf16(d_act * gate_pre * sigmoid_gate)
        g_gateup = jnp.stack([jnp.dot(normed_ffn.T, d_gate, preferred_element_type=jnp.float32), jnp.dot(normed_ffn.T, d_up, preferred_element_type=jnp.float32)])
        d_normed_ffn = tensor_sum([(d_gate, w_gu_b[0]), (d_up, w_gu_b[1])], hidden_width)
        d_res_norm, g_gain_ffn = norm_back(d_normed_ffn, residual, scale_ffn, gain_ffn)
        d_res = cot_rows + d_res_norm
        d_res_b = to_bf16(d_res)
        d_gated = jnp.dot(d_res_b, w_out_b, preferred_element_type=jnp.float32)
        g_out = jnp.dot(d_res_b.T, gated, preferred_element_type=jnp.float32)
        d_gate_c = d_gated * conv_out
        d_conv = d_gated * gate_c
        local_grad, edge_out = conv_back(d_conv, conv_taps, same_one, same_two)
        d_mixed = add_edge(local_grad, edge_in)
        g_taps = jnp.stack([lax.optimization_barrier(jnp.sum(d_conv * mixed_rows, axis=0)), lax.optimization_barrier(jnp.sum(same_one * d_conv * shift_one, axis=0)), lax.optimization_barrier(jnp.sum(same_two * d_conv * shift_two, axis=0))])
        d_b = to_bf16(d_mixed * gate_x)
        d_c = to_bf16(d_gate_c)
        d_x = to_bf16(d_mixed * gate_b)
        g_in = jnp.stack([jnp.dot(normed_mix.T, d_b, preferred_element_type=jnp.float32), jnp.dot(normed_mix.T, d_c, preferred_element_type=jnp.float32), jnp.dot(normed_mix.T, d_x, preferred_element_type=jnp.float32)])
        d_normed_mix = tensor_sum([(d_b, w_in_b[0]), (d_c, w_in_b[1]), (d_x, w_in_b[2])], chan_width)
        d_x_norm, g_gain_mix = norm_back(d_normed_mix, x_rows, scale_mix, gain_mix)
        grad_rows = d_res + d_x_norm
        parts = (g_gain_mix, g_gain_ffn, g_taps, g_in, g_out, g_gateup, g_down)
        sums_out = tuple((running + extra for running, extra in zip(sums_in, parts)))
        return ((edge_out, sums_out), (block_rows, grad_rows))
    zero_sums = (jnp.zeros((D,), jnp.float32), jnp.zeros((D,), jnp.float32), jnp.zeros((KW, D), jnp.float32), jnp.zeros((KW, D, D), jnp.float32), jnp.zeros((D, D), jnp.float32), jnp.zeros((2, D, FF), jnp.float32), jnp.zeros((D, FF), jnp.float32))
    start_carry = (jnp.zeros((2, D), jnp.float32), zero_sums)
    final_carry, outputs = lax.scan(block_step, start_carry, (x_blocks, id_blocks, cot_blocks, before_rows_all, before_ids_all), reverse=True)
    grad_gain_mix, grad_gain_ffn, grad_conv_taps, grad_w_inproj, grad_w_outproj, grad_w_gateup, grad_w_down = final_carry[1]
    block_out = outputs[0].reshape(TOKENS, D)
    grad_x = outputs[1].reshape(TOKENS, D)
    upd_gain_mix = adamw(gain_mix, grad_gain_mix, mean_gain_mix, var_gain_mix, rate_small, 0.0)
    upd_gain_ffn = adamw(gain_ffn, grad_gain_ffn, mean_gain_ffn, var_gain_ffn, rate_small, 0.0)
    upd_conv_taps = adamw(conv_taps, grad_conv_taps, mean_conv_taps, var_conv_taps, rate_small, 0.0)
    upd_w_inproj = adamw(w_inproj, grad_w_inproj, mean_w_inproj, var_w_inproj, rate_matrix, decay_matrix)
    upd_w_outproj = adamw(w_outproj, grad_w_outproj, mean_w_outproj, var_w_outproj, rate_matrix, decay_matrix)
    upd_w_gateup = adamw(w_gateup, grad_w_gateup, mean_w_gateup, var_w_gateup, rate_matrix, decay_matrix)
    upd_w_down = adamw(w_down, grad_w_down, mean_w_down, var_w_down, rate_matrix, decay_matrix)
    return (block_out, grad_x, grad_gain_mix, grad_gain_ffn, grad_conv_taps, grad_w_inproj, grad_w_outproj, grad_w_gateup, grad_w_down, upd_gain_mix[0], upd_gain_ffn[0], upd_conv_taps[0], upd_w_inproj[0], upd_w_outproj[0], upd_w_gateup[0], upd_w_down[0], upd_gain_mix[1], upd_gain_ffn[1], upd_conv_taps[1], upd_w_inproj[1], upd_w_outproj[1], upd_w_gateup[1], upd_w_down[1], upd_gain_mix[2], upd_gain_ffn[2], upd_conv_taps[2], upd_w_inproj[2], upd_w_outproj[2], upd_w_gateup[2], upd_w_down[2])
```

```python
import functools

import jax
import jax.numpy as jnp
from jax import lax
from jax.experimental import pallas as pl
from jax.experimental.pallas import tpu as pltpu
from jax.sharding import PartitionSpec as P

norm_eps = 1e-05
beta_one = 0.9
beta_two = 0.95
adam_eps = 1e-08
rate_matrix = 0.02
rate_small = 0.2
decay_matrix = 0.1
bias_one = 1.0 - 0.9**3
bias_two = 1.0 - 0.95**3


def flat_permute(value, pairs_of, n_dp, n_t):
    pairs = []
    for dp in range(n_dp):
        for t in range(n_t):
            target = pairs_of(dp, t)
            if target is not None:
                pairs.append((dp * n_t + t, target[0] * n_t + target[1]))
    return lax.ppermute(value, ("dp", "tensor"), pairs)


def token_shift(value, steps, n_dp, n_t):
    count = n_dp * n_t
    pairs = [(i, i + steps) for i in range(count) if 0 <= i + steps < count]
    return lax.ppermute(value, ("dp", "tensor"), pairs)


def sum_everywhere(value, n_dp, n_t):
    count = n_dp * n_t
    if count & (count - 1):
        return lax.psum(value, ("dp", "tensor"))
    bit = 1
    while bit < count:
        value = value + lax.ppermute(value, ("dp", "tensor"), [(i, i ^ bit) for i in range(count)])
        bit *= 2
    return value


def first_axis(t):
    return 2 if t % 2 == 0 else 1


def scatter_sum(parts, n_dp, n_t):
    f32 = jnp.float32
    total = parts[0].astype(f32)
    for r in range(1, n_t):
        got = flat_permute(parts[r], lambda dp, t: (dp, (t + r) % n_t), n_dp, n_t)
        total = total + got.astype(f32)
    planes, rows, width = total.shape
    n_z = n_dp // 4
    blocks = total.astype(jnp.bfloat16).reshape(planes, n_z, 4, rows // n_dp, width)
    dp = lax.axis_index("dp")
    odd = lax.rem(lax.axis_index("tensor"), 2)
    quad = lax.rem(dp, 4)
    bit_x = lax.rem(quad, 2)
    bit_y = quad // 2
    by_x = quad + 1 - 2 * bit_x
    by_y = quad + 2 - 4 * bit_y
    first = (1 - odd) * by_y + odd * by_x
    second = (1 - odd) * by_x + odd * by_y
    far = 3 - quad

    def pick(value, index):
        return lax.dynamic_slice_in_dim(value, index, 1, 2)

    send = jnp.concatenate([pick(blocks, first), pick(blocks, far)], axis=2)
    got = flat_permute(send, lambda dp, t: (dp ^ first_axis(t), t), n_dp, n_t).astype(f32)
    mine = pick(blocks, quad).astype(f32) + got[:, :, 0:1]
    send = (pick(blocks, second).astype(f32) + got[:, :, 1:2]).astype(jnp.bfloat16)
    got = flat_permute(send, lambda dp, t: (dp ^ (3 - first_axis(t)), t), n_dp, n_t).astype(f32)
    column = (mine + got)[:, :, 0]
    z = dp // 4
    result = lax.dynamic_slice_in_dim(column, z, 1, 1)
    column = column.astype(jnp.bfloat16)
    for k in range(1, n_z):
        send = lax.dynamic_slice_in_dim(column, lax.rem(z + k, n_z), 1, 1)
        result = result + flat_permute(
            send, lambda dp, t: ((dp + 4 * k) % n_dp, t), n_dp, n_t
        ).astype(f32)
    return result[:, 0]


def rms_scale(values):
    return lax.rsqrt(jnp.mean(values * values, axis=1, keepdims=True) + norm_eps)


def norm_back(d_normed, values, scale_rows, gain):
    gain_part = jnp.sum(d_normed * values * scale_rows, axis=0)
    scaled = d_normed * gain
    inner = jnp.mean(scaled * values, axis=1, keepdims=True)
    return (scale_rows * (scaled - values * scale_rows * scale_rows * inner), gain_part)


def adamw(weight, gradient, moment, square, step_size, weight_decay):
    new_moment = beta_one * moment + (1.0 - beta_one) * gradient
    new_square = beta_two * square + (1.0 - beta_two) * gradient * gradient
    direction = new_moment / bias_one / (jnp.sqrt(new_square / bias_two) + adam_eps)
    return (weight - step_size * (direction + weight_decay * weight), new_moment, new_square)


MESH = pl.DeviceIdType.MESH

def gather_kernel(n_dp, n_t, chunks, *refs):
    n_w = len(set(c[0] for c in chunks))
    shards = refs[:n_w]
    outs = refs[n_w:2*n_w]
    loc, zs, zr, as_, ar, bs, br, cs, cr = refs[2*n_w:]
    n_z = n_dp // 4
    dp = lax.axis_index("dp"); t = lax.axis_index("tensor")
    x = lax.rem(dp, 2); y = lax.rem(dp // 2, 2); z = dp // 4
    par = lax.rem(t, 2)
    x_dp = dp + 1 - 2 * x
    y_dp = dp + 2 - 4 * y
    a_dp = (1 - par) * x_dp + par * y_dp
    b_dp = par * x_dp + (1 - par) * y_dp
    q = lax.rem(dp, 4)
    qa = lax.rem(a_dp, 4)
    z_to = [lax.rem(z + k, n_z) * 4 + q for k in range(1, n_z)]
    t_to = [lax.rem(t + n_t - r, n_t) for r in range(1, n_t)]
    barrier = pltpu.get_barrier_semaphore()
    peers = [(d, t) for d in z_to] + [(a_dp, t), (b_dp, t)] + [(dp, u) for u in t_to]
    for peer in peers:
        pl.semaphore_signal(barrier, inc=1, device_id=peer, device_id_type=MESH)
    pl.semaphore_wait(barrier, len(peers))

    def src_own(c):
        w, k = chunks[c]
        return shards[w].at[k]
    def blk(c, i, slot=0):
        w, k = chunks[c]
        return outs[w].at[slot, k, i]
    def rc(src, dst, ss, rs, dev):
        return pltpu.make_async_remote_copy(src_ref=src, dst_ref=dst, send_sem=ss, recv_sem=rs, device_id=dev, device_id_type=MESH)
    me = dp
    col = [lax.rem(z + n_z - k, n_z) * 4 for k in range(n_z)]
    n_c = len(chunks)
    started = []
    def start(d):
        d.start(); started.append(d)
    locs = []
    for c in range(n_c):
        l = pltpu.make_async_copy(src_own(c), blk(c, me), loc.at[c]); l.start(); locs.append(l)
        for k in range(1, n_z):
            start(rc(src_own(c), blk(c, me), zs.at[c, k - 1], zr.at[c, k - 1], (z_to[k - 1], t)))
    for s in range(n_c + 3):
        c = s
        if c < n_c:
            for k in range(n_z):
                if k == 0:
                    src = src_own(c)
                else:
                    src = blk(c, col[k] + q)
                    rc(src, src, zs.at[c, k - 1], zr.at[c, k - 1], (dp, t)).wait_recv()
                start(rc(src, blk(c, col[k] + q), as_.at[c, k], ar.at[c, k], (a_dp, t)))
                start(rc(src, blk(c, col[k] + q), bs.at[c, k], br.at[c, k], (b_dp, t)))
        c = s - 1
        if 0 <= c < n_c:
            for k in range(n_z):
                src = blk(c, col[k] + qa)
                rc(src, src, as_.at[c, k], ar.at[c, k], (dp, t)).wait_recv()
                start(rc(src, src, bs.at[c, n_z + k], br.at[c, n_z + k], (b_dp, t)))
        c = s - 2
        if 0 <= c < n_c:
            w, kk = chunks[c]
            for k in range(2 * n_z):
                src = blk(c, me)
                rc(src, src, bs.at[c, k], br.at[c, k], (dp, t)).wait_recv()
            locs[c].wait()
            for r in range(1, n_t):
                start(rc(outs[w].at[0, kk], outs[w].at[r, kk], cs.at[c, r - 1], cr.at[c, r - 1], (dp, t_to[r - 1])))
        c = s - 3
        if 0 <= c < n_c:
            w, kk = chunks[c]
            for r in range(1, n_t):
                rc(outs[w].at[0, kk], outs[w].at[r, kk], cs.at[c, r - 1], cr.at[c, r - 1], (dp, t)).wait_recv()
    for d in started:
        d.wait_send()

def gather_all(shards, n_dp, n_t, cid=1):
    chunks = [(w, k) for w, s in enumerate(shards) for k in range(s.shape[0])]
    n_c = len(chunks); n_z = n_dp // 4
    DMA = pltpu.SemaphoreType.DMA
    return pl.pallas_call(
        functools.partial(gather_kernel, n_dp, n_t, chunks),
        out_shape=[jax.ShapeDtypeStruct((n_t, s.shape[0], n_dp) + s.shape[1:], s.dtype) for s in shards],
        in_specs=[pl.BlockSpec(memory_space=pltpu.VMEM)] * len(shards),
        out_specs=[pl.BlockSpec(memory_space=pl.ANY)] * len(shards),
        scratch_shapes=[DMA((n_c,)), DMA((n_c, n_z - 1)), DMA((n_c, n_z - 1)), DMA((n_c, n_z)), DMA((n_c, n_z)),
                        DMA((n_c, 2 * n_z)), DMA((n_c, 2 * n_z)), DMA((n_c, max(1, n_t - 1))), DMA((n_c, max(1, n_t - 1)))],
        compiler_params=pltpu.CompilerParams(collective_id=cid, has_side_effects=True),
        name="gather_all",
    )(*shards)


def per_device(
    x_in,
    segment_ids,
    cotangent,
    gain_mix,
    mean_gain_mix,
    var_gain_mix,
    gain_ffn,
    mean_gain_ffn,
    var_gain_ffn,
    conv_taps,
    mean_conv_taps,
    var_conv_taps,
    w_inproj,
    mean_w_inproj,
    var_w_inproj,
    w_outproj,
    mean_w_outproj,
    var_w_outproj,
    w_gateup,
    mean_w_gateup,
    var_w_gateup,
    w_down,
    mean_w_down,
    var_w_down,
):
    bf16 = jnp.bfloat16
    f32 = jnp.float32
    n_dp = lax.axis_size("dp")
    n_t = lax.axis_size("tensor")
    t_index = lax.axis_index("tensor")
    chan_count = conv_taps.shape[1]
    width_full = gain_mix.shape[0]
    token_count = x_in.shape[0]

    gathered = gather_all(
        [
            w_inproj.astype(bf16),
            w_outproj.astype(bf16)[None],
            w_gateup.astype(bf16),
            w_down.astype(bf16)[None],
        ],
        n_dp,
        n_t,
    )
    w_in_full, w_out_full, w_gu_full, w_down_full = (
        g.reshape(g.shape[:2] + (g.shape[2] * g.shape[3], g.shape[4])) for g in gathered
    )
    w_out_full = w_out_full[:, 0]
    w_down_full = w_down_full[:, 0]
    taps = jnp.stack(
        [conv_taps]
        + [
            lax.ppermute(conv_taps, "tensor", [((i + r) % n_t, i) for i in range(n_t)])
            for r in range(1, n_t)
        ],
        axis=1,
    )[:, :, None, :]

    scale_mix = rms_scale(x_in)
    normed_mix = (x_in * scale_mix * gain_mix).astype(bf16)
    projected = jnp.einsum("td,skdc->kstc", normed_mix, w_in_full, preferred_element_type=f32)
    gate_b = projected[0]
    gate_c = projected[1]
    gate_x = projected[2]
    mixed_rows = gate_b * gate_x
    ids_float = lax.dynamic_slice_in_dim(segment_ids, t_index * token_count, token_count).astype(f32)
    prev_ids = token_shift(ids_float[token_count - 2 :], 1, n_dp, n_t)
    prev_u = token_shift(jnp.roll(mixed_rows[:, token_count - 2 :], -1, axis=0), 1, n_dp, n_t)
    ext_u = jnp.concatenate([prev_u, mixed_rows], axis=1)
    ext_ids = jnp.concatenate([prev_ids, ids_float], axis=0)
    same_one = (ext_ids[1 : token_count + 1] == ids_float).astype(f32)[:, None]
    same_two = (ext_ids[0:token_count] == ids_float).astype(f32)[:, None]
    shift_one = ext_u[:, 1 : token_count + 1]
    shift_two = ext_u[:, 0:token_count]
    conv_out = (
        taps[0] * mixed_rows + taps[1] * same_one * shift_one + taps[2] * same_two * shift_two
    )
    gated = (gate_c * conv_out).astype(bf16)
    residual = x_in + jnp.einsum("stc,sdc->td", gated, w_out_full, preferred_element_type=f32)
    scale_ffn = rms_scale(residual)
    normed_ffn = (residual * scale_ffn * gain_ffn).astype(bf16)
    gate_up = jnp.einsum("td,skdf->kstf", normed_ffn, w_gu_full, preferred_element_type=f32)
    gate_pre = gate_up[0]
    up_pre = gate_up[1]
    sigmoid_gate = jax.nn.sigmoid(gate_pre)
    activated = (gate_pre * sigmoid_gate * up_pre).astype(bf16)
    cot_b = cotangent.astype(bf16)
    down_parts = [
        jnp.einsum("td,tf->df", cot_b, activated[r], preferred_element_type=f32).astype(bf16)[None]
        for r in range(n_t)
    ]
    grad_down_shard = scatter_sum(down_parts, n_dp, n_t)[0]
    block_out = residual + jnp.einsum(
        "stf,sdf->td", activated, w_down_full, preferred_element_type=f32
    )
    d_act = jnp.einsum("td,sdf->stf", cot_b, w_down_full, preferred_element_type=f32)
    d_gate = d_act * up_pre * sigmoid_gate * (1.0 + gate_pre * (1.0 - sigmoid_gate))
    d_up = d_act * gate_pre * sigmoid_gate
    d_gateup = jnp.stack([d_gate, d_up]).astype(bf16)
    gu_parts = [
        jnp.einsum("td,ktf->kdf", normed_ffn, d_gateup[:, r], preferred_element_type=f32).astype(
            bf16
        )
        for r in range(n_t)
    ]
    grad_gu_shard = scatter_sum(gu_parts, n_dp, n_t)
    d_normed_ffn = jnp.einsum("kstf,skdf->td", d_gateup, w_gu_full, preferred_element_type=f32)
    d_res_norm, ffn_gain_part = norm_back(d_normed_ffn, residual, scale_ffn, gain_ffn)
    d_res = cotangent + d_res_norm
    d_res_b = d_res.astype(bf16)
    d_gated = jnp.einsum("td,sdc->stc", d_res_b, w_out_full, preferred_element_type=f32)
    d_gate_c = d_gated * conv_out
    d_conv = d_gated * gate_c
    term_zero = taps[0] * d_conv
    term_one = taps[1] * same_one * d_conv
    term_two = taps[2] * same_two * d_conv
    edge_out = jnp.stack([term_two[:, 0], term_one[:, 0] + term_two[:, 1]], axis=1)
    edge_in = token_shift(jnp.roll(edge_out, 1, axis=0), -1, n_dp, n_t)
    zero_row = jnp.zeros_like(edge_in[:, :1])
    d_mixed = (
        term_zero
        + jnp.concatenate([term_one[:, 1:], zero_row], axis=1)
        + jnp.concatenate([term_two[:, 2:], edge_in], axis=1)
    )
    taps_part = jnp.stack(
        [
            jnp.sum(d_conv * mixed_rows, axis=1),
            jnp.sum(same_one * d_conv * shift_one, axis=1),
            jnp.sum(same_two * d_conv * shift_two, axis=1),
        ]
    )
    d_proj = jnp.stack([d_mixed * gate_x, d_gate_c, d_mixed * gate_b]).astype(bf16)
    conv_parts = [
        jnp.concatenate(
            [
                jnp.einsum("td,ktc->kdc", normed_mix, d_proj[:, r], preferred_element_type=f32),
                jnp.einsum("td,tc->dc", d_res_b, gated[r], preferred_element_type=f32)[None],
            ]
        ).astype(bf16)
        for r in range(n_t)
    ]
    conv_shard = scatter_sum(conv_parts, n_dp, n_t)
    grad_in_shard = conv_shard[:-1]
    grad_out_shard = conv_shard[-1]
    d_normed_mix = jnp.einsum("kstc,skdc->td", d_proj, w_in_full, preferred_element_type=f32)
    d_x_norm, mix_gain_part = norm_back(d_normed_mix, x_in, scale_mix, gain_mix)
    grad_x = d_res + d_x_norm
    taps_placed = jnp.zeros((taps_part.shape[0], width_full), f32)
    for r in range(n_t):
        taps_placed = lax.dynamic_update_slice(
            taps_placed, taps_part[:, r], (jnp.int32(0), lax.rem(t_index + r, n_t) * chan_count)
        )
    small_total = sum_everywhere(
        jnp.concatenate([mix_gain_part[None], ffn_gain_part[None], taps_placed]), n_dp, n_t
    )
    grad_gain_mix = small_total[0]
    grad_gain_ffn = small_total[1]
    grad_conv_taps = lax.dynamic_slice_in_dim(small_total[2:], t_index * chan_count, chan_count, 1)
    upd_gain_mix = adamw(gain_mix, grad_gain_mix, mean_gain_mix, var_gain_mix, rate_small, 0.0)
    upd_gain_ffn = adamw(gain_ffn, grad_gain_ffn, mean_gain_ffn, var_gain_ffn, rate_small, 0.0)
    upd_conv_taps = adamw(conv_taps, grad_conv_taps, mean_conv_taps, var_conv_taps, rate_small, 0.0)
    upd_w_inproj = adamw(
        w_inproj, grad_in_shard, mean_w_inproj, var_w_inproj, rate_matrix, decay_matrix
    )
    upd_w_outproj = adamw(
        w_outproj, grad_out_shard, mean_w_outproj, var_w_outproj, rate_matrix, decay_matrix
    )
    upd_w_gateup = adamw(
        w_gateup, grad_gu_shard, mean_w_gateup, var_w_gateup, rate_matrix, decay_matrix
    )
    upd_w_down = adamw(w_down, grad_down_shard, mean_w_down, var_w_down, rate_matrix, decay_matrix)
    return (
        block_out,
        grad_x,
        grad_gain_mix,
        grad_gain_ffn,
        grad_conv_taps,
        grad_in_shard,
        grad_out_shard,
        grad_gu_shard,
        grad_down_shard,
        upd_gain_mix[0],
        upd_gain_ffn[0],
        upd_conv_taps[0],
        upd_w_inproj[0],
        upd_w_outproj[0],
        upd_w_gateup[0],
        upd_w_down[0],
        upd_gain_mix[1],
        upd_gain_ffn[1],
        upd_conv_taps[1],
        upd_w_inproj[1],
        upd_w_outproj[1],
        upd_w_gateup[1],
        upd_w_down[1],
        upd_gain_mix[2],
        upd_gain_ffn[2],
        upd_conv_taps[2],
        upd_w_inproj[2],
        upd_w_outproj[2],
        upd_w_gateup[2],
        upd_w_down[2],
    )


def solution(mesh):
    in_specs = (
        P(("dp", "tensor"), None),
        P("dp"),
        P(("dp", "tensor"), None),
        P(),
        P(),
        P(),
        P(),
        P(),
        P(),
        P(None, "tensor"),
        P(None, "tensor"),
        P(None, "tensor"),
        P(None, "dp", "tensor"),
        P(None, "dp", "tensor"),
        P(None, "dp", "tensor"),
        P("dp", "tensor"),
        P("dp", "tensor"),
        P("dp", "tensor"),
        P(None, "dp", "tensor"),
        P(None, "dp", "tensor"),
        P(None, "dp", "tensor"),
        P("dp", "tensor"),
        P("dp", "tensor"),
        P("dp", "tensor"),
    )
    out_specs = (
        P(("dp", "tensor"), None),
        P(("dp", "tensor"), None),
        P(),
        P(),
        P(None, "tensor"),
        P(None, "dp", "tensor"),
        P("dp", "tensor"),
        P(None, "dp", "tensor"),
        P("dp", "tensor"),
        P(),
        P(),
        P(None, "tensor"),
        P(None, "dp", "tensor"),
        P("dp", "tensor"),
        P(None, "dp", "tensor"),
        P("dp", "tensor"),
        P(),
        P(),
        P(None, "tensor"),
        P(None, "dp", "tensor"),
        P("dp", "tensor"),
        P(None, "dp", "tensor"),
        P("dp", "tensor"),
        P(),
        P(),
        P(None, "tensor"),
        P(None, "dp", "tensor"),
        P("dp", "tensor"),
        P(None, "dp", "tensor"),
        P("dp", "tensor"),
    )
    return jax.shard_map(
        per_device, mesh=mesh, in_specs=in_specs, out_specs=out_specs, check_vma=False
    )
```
